32 devices in a mesh: dp: 2 (over core), tensor: 16 (over z, y, x).
Axes of the slice: x: 2, y: 2, z: 4, core: 2. Of those that a mesh axis runs over, the one named last changes fastest.
Arguments:
- gradient: float32 [2, 8192, 512], P('dp', 'tensor'), may hold values from -80 to 80
Outputs:
- update: bfloat16 [2, 8192, 512], P(None, 'tensor')
The draws below stay inside these ranges and needn't reach their ends.
All inputs are finite; a program needn't handle non-finite values.
Results may differ from the reference program's by a relative error of at most 0.001.
Values may be sent and summed in bfloat16 or wider, within the bound.
A program may use at most 64 MiB of HBM per device.

```python
import math
import jax
import jax.numpy as jnp
from jax import lax

FEATURES = 8192
OUTPUTS = 512
ITERS = 3
MATS = 2


def draw_gradient(key, part):
    keys = jax.random.split(jax.random.fold_in(key, 17), 5)
    ramp = 1.0 + 2.0 * jnp.arange(FEATURES, dtype=jnp.float32) / (FEATURES - 1)
    feature_scale = jnp.exp(jax.random.uniform(keys[0], (MATS, FEATURES, 1), jnp.float32, 0.0, math.log(10.0))) * ramp[None, :, None]
    output_scale = jnp.exp(jax.random.uniform(keys[1], (MATS, 1, OUTPUTS), jnp.float32, 0.0, math.log(10.0)))
    common = jax.random.truncated_normal(keys[2], -6.0, 6.0, (MATS, 1, OUTPUTS), jnp.float32)
    bulk = jax.random.truncated_normal(keys[4], -6.0, 6.0, (MATS, FEATURES, OUTPUTS), jnp.float32)
    return 0.01 * feature_scale * output_scale * (bulk + 0.35 * common)


def setup_inputs(seed: int = 0) -> dict:
    key_of = jax.random.split(jax.random.key(seed), 2)
    gradient = draw_gradient(jax.random.fold_in(key_of[1], 71), 0)
    return dict(gradient=gradient)


linear_term = 3.4445
cubic_term = -4.775
quintic_term = 2.0315
norm_floor = 1e-07
update_gain = 0.2

def multiply(first_factor, second_factor):
    return jnp.einsum('mrs,mst->mrt', first_factor, second_factor, precision=lax.Precision.HIGHEST)

def reference(gradient):
    squared_norm = lax.optimization_barrier(jnp.sum(gradient * gradient, axis=(1, 2)))
    divisor = jnp.sqrt(squared_norm) + norm_floor
    raw_gram = jnp.einsum('mfr,mfs->mrs', gradient, gradient, precision=lax.Precision.HIGHEST)
    gram_matrix = raw_gram / (divisor * divisor)[:, None, None]
    identity = jnp.eye(OUTPUTS, dtype=jnp.float32)[None]
    running = identity
    for turn_index in range(ITERS):
        squared = multiply(gram_matrix, gram_matrix)
        polynomial = linear_term * identity + cubic_term * gram_matrix + quintic_term * squared
        if turn_index == 0:
            running = polynomial
        else:
            running = multiply(running, polynomial)
        if turn_index + 1 < ITERS:
            gram_matrix = multiply(multiply(polynomial, gram_matrix), polynomial)
    polished = jnp.einsum('mfr,mrs->mfs', gradient, running, precision=lax.Precision.HIGHEST)
    factor = update_gain * math.sqrt(max(FEATURES, OUTPUTS)) / divisor
    return (factor[:, None, None] * polished).astype(jnp.bfloat16)
```

```python
import functools
import math

import jax
import jax.numpy as jnp
from jax import lax
from jax.experimental import pallas as pl
from jax.experimental.pallas import tpu as pltpu
from jax.sharding import PartitionSpec as P

ITERS = 3
BLOCK = 128

linear_term = 3.4445
cubic_term = -4.775
quintic_term = 2.0315
norm_floor = 1e-07
update_gain = 0.2

MESH = pl.DeviceIdType.MESH


def block_pairs(order):
    count = order // BLOCK
    return [(i, j) for i in range(count) for j in range(i, count)]


def split(value):
    high = value.astype(jnp.bfloat16)
    return high, (value - high.astype(jnp.float32)).astype(jnp.bfloat16)


def dot(a, b):
    return lax.dot_general(a, b, (((1,), (0,)), ((), ())), preferred_element_type=jnp.float32)


def kernel(
    shape, g_ref, out_ref, gt, raw, part, recv_in, stage, recv_out, full, gram, lhs, gsplit,
    p0s, ps, qs, gs, s1, r1, s2, r2, s3, r3, s4, r4, s5, r5,
):
    ndp, n_in, n_out, rows, order, chunk = shape
    tile = min(256, rows)
    mtile = min(256, order)
    dp = lax.axis_index("dp")
    tensor = lax.axis_index("tensor")
    ti, to = lax.rem(tensor, n_in), lax.div(tensor, n_in)

    def inner(d):
        return lax.rem(ti + d, n_in)

    def outer(e):
        return lax.rem(to + e, n_out)

    def rank(i, o):
        return o * n_in + i

    def span(i, o):
        return pl.ds(pl.multiple_of((i * n_out + o) * chunk, 8), chunk)

    barrier = pltpu.get_barrier_semaphore()
    for d in range(1, n_in):
        pl.semaphore_signal(barrier, inc=1, device_id=(dp, rank(inner(d), to)), device_id_type=MESH)
    for e in range(1, n_out):
        pl.semaphore_signal(barrier, inc=1, device_id=(dp, rank(ti, outer(e))), device_id_type=MESH)
    for d in range(1, ndp):
        pl.semaphore_signal(
            barrier, inc=1, device_id=(lax.rem(dp + d, ndp), tensor), device_id_type=MESH
        )

    def put(ref, at, value):
        high, low = split(value)
        ref[0, at, :] = high
        ref[1, at, :] = low

    for r in range(0, rows, tile):
        put(gsplit, pl.ds(r, tile), g_ref[pl.ds(r, tile), :])
    turned = g_ref[...].T
    high, low = split(turned)
    gt[0] = high
    gt[1] = low
    for r in range(0, order, mtile):
        at = pl.ds(r, mtile)
        raw[at, :] = (
            dot(gt[0, at, :], gsplit[1]) + dot(gt[1, at, :], gsplit[0])
        ) + dot(gt[0, at, :], gsplit[0])

    pairs = block_pairs(order)
    for b, (i, j) in enumerate(pairs):
        part[pl.ds(b * BLOCK, BLOCK), :] = raw[
            pl.ds(i * BLOCK, BLOCK), pl.ds(j * BLOCK, BLOCK)
        ]
    total_rows = part.shape[0]
    if total_rows > len(pairs) * BLOCK:
        pad = total_rows - len(pairs) * BLOCK
        part[pl.ds(len(pairs) * BLOCK, pad), :] = jnp.zeros((pad, BLOCK), jnp.float32)

    pl.semaphore_wait(barrier, (n_in - 1) + (n_out - 1) + (ndp - 1))

    def remote(src, dst, send, recv, device):
        return pltpu.make_async_remote_copy(
            src_ref=src, dst_ref=dst, send_sem=send, recv_sem=recv,
            device_id=device, device_id_type=MESH,
        )

    turns = list(range(1, n_out))[::-1] + [0]
    first = {}
    for e in turns:
        for d in range(1, n_in):
            copy = remote(
                part.at[span(inner(d), outer(e)), :], recv_in.at[d - 1, e],
                s1.at[d - 1, e], r1.at[d - 1, e], (dp, rank(inner(d), to)),
            )
            copy.start()
            first[d, e] = copy
    second = {}
    for e in turns:
        value = part[span(ti, outer(e)), :]
        for d in range(1, n_in):
            first[d, e].wait_recv()
            value = value + recv_in[d - 1, e]
        if e:
            stage[e - 1] = value
            copy = remote(
                stage.at[e - 1], recv_out.at[e - 1], s2.at[e - 1], r2.at[e - 1],
                (dp, rank(ti, outer(e))),
            )
            copy.start()
            second[e] = copy
    for e in range(1, n_out):
        second[e].wait_recv()
        value = value + recv_out[e - 1]
    full[span(ti, to), :] = value

    third, fourth = {}, {}
    mine = full.at[span(ti, to), :]
    for e in turns[:-1]:
        copy = remote(mine, mine, s3.at[e - 1], r3.at[e - 1], (dp, rank(ti, outer(e))))
        copy.start()
        third[e] = copy

    def pass_on(e):
        block = full.at[span(ti, lax.rem(to - e + n_out, n_out)), :]
        for d in range(1, n_in):
            copy = remote(
                block, block, s4.at[d - 1, e], r4.at[d - 1, e], (dp, rank(inner(d), to))
            )
            copy.start()
            fourth[d, e] = copy

    pass_on(0)
    for e in range(1, n_out):
        third[e].wait_recv()
        pass_on(e)
    for e in range(n_out):
        for d in range(1, n_in):
            fourth[d, e].wait_recv()

    here = lax.broadcasted_iota(jnp.int32, (BLOCK, BLOCK), 0)
    there = lax.broadcasted_iota(jnp.int32, (BLOCK, BLOCK), 1)
    squared = jnp.zeros((BLOCK, BLOCK), jnp.float32)
    for b, (i, j) in enumerate(pairs):
        if i == j:
            squared = squared + jnp.where(here == there, full[pl.ds(b * BLOCK, BLOCK), :], 0.0)
    squared_norm = jnp.sum(jnp.sum(squared, axis=1, keepdims=True), axis=0, keepdims=True)
    divisor = jnp.sqrt(squared_norm) + norm_floor
    scale = 1.0 / (divisor * divisor)
    for b, (i, j) in enumerate(pairs):
        value = full[pl.ds(b * BLOCK, BLOCK), :] * scale
        gram[pl.ds(i * BLOCK, BLOCK), pl.ds(j * BLOCK, BLOCK)] = value
        if i != j:
            gram[pl.ds(j * BLOCK, BLOCK), pl.ds(i * BLOCK, BLOCK)] = value.T

    def product(a, b, at):
        return (
            dot(a[0, at, :], b[1]) + dot(a[1, at, :], b[0])
        ) + dot(a[0, at, :], b[0])

    def polynomial(grams, target):
        for r in range(0, order, mtile):
            at = pl.ds(r, mtile)
            row = lax.broadcasted_iota(jnp.int32, (mtile, order), 0) + r
            column = lax.broadcasted_iota(jnp.int32, (mtile, order), 1)
            value = cubic_term * gram[at, :] + quintic_term * product(grams, grams, at)
            put(target, at, value + jnp.where(row == column, linear_term, 0.0))

    def multiply(a, b, target, keep=None):
        for r in range(0, order, mtile):
            at = pl.ds(r, mtile)
            value = product(a, b, at)
            if keep is not None:
                keep[at, :] = value
            put(target, at, value)

    for r in range(0, order, mtile):
        put(gs, pl.ds(r, mtile), gram[pl.ds(r, mtile), :])
    running, spare = p0s, lhs
    for turn in range(ITERS):
        target = running if turn == 0 else ps
        polynomial(gs, target)
        if turn + 1 < ITERS:
            multiply(target, gs, qs)
            multiply(qs, target, gs, gram)
        if turn > 0:
            multiply(running, target, spare)
            running, spare = spare, running

    factor = update_gain * math.sqrt(max(rows * n_in * n_out, order)) / divisor
    last = []
    for k, r in enumerate(range(0, rows, tile)):
        at = pl.ds(r, tile)
        out_ref[dp, at, :] = (product(gsplit, running, at) * factor).astype(jnp.bfloat16)
        block = out_ref.at[dp, at, :]
        for d in range(1, ndp):
            copy = remote(
                block, block, s5.at[d - 1, k], r5.at[d - 1, k], (lax.rem(dp + d, ndp), tensor)
            )
            copy.start()
            last.append(copy)
    for copy in list(first.values()) + list(second.values()) + list(third.values()):
        copy.wait_send()
    for copy in fourth.values():
        copy.wait_send()
    for copy in last:
        copy.wait()


def on_device(ndp, n, gradient):
    rows, order = gradient.shape[1], gradient.shape[2]
    n_in = 4 if n % 4 == 0 else 1
    n_out = n // n_in
    tile = min(256, rows)
    pieces = rows // tile
    packed = len(block_pairs(order)) * BLOCK
    chunk = -(-packed // (8 * n)) * 8
    total = chunk * n
    shape = (ndp, n_in, n_out, rows, order, chunk)
    bf, f32 = jnp.bfloat16, jnp.float32
    inner, outer = max(n_in - 1, 1), max(n_out - 1, 1)
    dma = pltpu.SemaphoreType.DMA
    pair = pltpu.VMEM((2, order, order), bf)
    return pl.pallas_call(
        functools.partial(kernel, shape),
        out_shape=jax.ShapeDtypeStruct((ndp, rows, order), bf),
        in_specs=[pl.BlockSpec(memory_space=pltpu.VMEM)],
        out_specs=pl.BlockSpec(memory_space=pltpu.VMEM),
        scratch_shapes=[
            pltpu.VMEM((2, order, rows), bf),
            pltpu.VMEM((order, order), f32),
            pltpu.VMEM((total, BLOCK), f32),
            pltpu.VMEM((inner, n_out, chunk, BLOCK), f32),
            pltpu.VMEM((outer, chunk, BLOCK), f32),
            pltpu.VMEM((outer, chunk, BLOCK), f32),
            pltpu.VMEM((total, BLOCK), f32),
            pltpu.VMEM((order, order), f32),
            pair,
            pltpu.VMEM((2, rows, order), bf),
            pair,
            pair,
            pair,
            pair,
            dma((inner, n_out)),
            dma((inner, n_out)),
            dma((outer,)),
            dma((outer,)),
            dma((outer,)),
            dma((outer,)),
            dma((inner, n_out)),
            dma((inner, n_out)),
            dma((max(ndp - 1, 1), pieces)),
            dma((max(ndp - 1, 1), pieces)),
        ],
        compiler_params=pltpu.CompilerParams(
            collective_id=0, has_side_effects=True, vmem_limit_bytes=48 * 1024 * 1024
        ),
    )(gradient[0])


def solution(mesh):
    body = functools.partial(on_device, mesh.shape["dp"], mesh.shape["tensor"])
    return jax.shard_map(
        body, mesh=mesh, in_specs=(P("dp", "tensor", None),),
        out_specs=P(None, "tensor", None), check_vma=False,
    )
```

```python
import functools
import math

import jax
import jax.numpy as jnp
from jax import lax
from jax.experimental import pallas as pl
from jax.experimental.pallas import tpu as pltpu
from jax.sharding import PartitionSpec as P

ITERS = 3
BLOCK = 128
CUT = 4

linear_term = 3.4445
cubic_term = -4.775
quintic_term = 2.0315
norm_floor = 1e-07
update_gain = 0.2

MESH = pl.DeviceIdType.MESH


def split(value):
    high = value.astype(jnp.bfloat16)
    return high, (value - high.astype(jnp.float32)).astype(jnp.bfloat16)


def dot(a, b):
    return lax.dot_general(a, b, (((1,), (0,)), ((), ())), preferred_element_type=jnp.float32)


def kernel(
    shape, g_hbm, out_ref, g_ref, gt, raw, part, full, gram, spare, gsplit, p0s, ps, qs, gs,
    dtile, dgot_in, dgot_out, in_a, hold_a, out_a, in_b, hold_b, out_b,
    gsem, d1, d2, d3, d4, sems_a, sems_b, s5, r5,
):
    ndp, n_in, n_out, rows, order, chunk, cut = shape
    tile = min(256, rows)
    mtile = min(256, order)
    dp = lax.axis_index("dp")
    tensor = lax.axis_index("tensor")
    ti, to = lax.rem(tensor, n_in), lax.div(tensor, n_in)

    def inner(d):
        return dp, to * n_in + lax.rem(ti + d, n_in)

    def outer(e):
        return dp, lax.rem(to + e, n_out) * n_in + ti

    def sibling(d):
        return lax.rem(dp + d, ndp), tensor

    barrier = pltpu.get_barrier_semaphore()
    for d in range(1, n_in):
        pl.semaphore_signal(barrier, inc=1, device_id=inner(d), device_id_type=MESH)
    for e in range(1, n_out):
        pl.semaphore_signal(barrier, inc=1, device_id=outer(e), device_id_type=MESH)
    for d in range(1, ndp):
        pl.semaphore_signal(barrier, inc=1, device_id=sibling(d), device_id_type=MESH)

    def put(ref, at, columns, value):
        high, low = split(value)
        ref[0, at, columns] = high
        ref[1, at, columns] = low

    every = pl.ds(0, order)
    loads = []
    for k, r in enumerate(range(0, rows, tile)):
        at = pl.ds(r, tile)
        copy = pltpu.make_async_copy(g_hbm.at[at, :], g_ref.at[at, :], gsem.at[k])
        copy.start()
        loads.append(copy)
    for k, r in enumerate(range(0, rows, tile)):
        at = pl.ds(r, tile)
        loads[k].wait()
        value = g_ref[at, :]
        put(gsplit, at, every, value)
        put(gt, every, at, value.T)
    for r in range(0, order, mtile):
        at, columns = pl.ds(r, mtile), pl.ds(r, order - r)
        raw[at, columns] = (
            dot(gt[0, at, :], gsplit[1, :, columns]) + dot(gt[1, at, :], gsplit[0, :, columns])
        ) + dot(gt[0, at, :], gsplit[0, :, columns])

    here = lax.broadcasted_iota(jnp.int32, (BLOCK, BLOCK), 0)
    there = lax.broadcasted_iota(jnp.int32, (BLOCK, BLOCK), 1)
    above, diagonal = here <= there, here == there

    def block(i, j):
        return pl.ds(i * BLOCK, BLOCK), pl.ds(j * BLOCK, BLOCK)

    count = order // BLOCK
    pairs = [(i, j) for i in range(count) for j in range(i + 1, count)]
    for b, (i, j) in enumerate(pairs):
        part[block(b, 0)] = raw[block(i, j)]
    dtile[...] = jnp.zeros_like(dtile)
    for m in range(count // 2):
        one, two = raw[block(2 * m, 2 * m)], raw[block(2 * m + 1, 2 * m + 1)]
        part[block(len(pairs) + m, 0)] = jnp.where(above, one, two)
        dtile[0, pl.ds(m, 1), :] = jnp.sum(jnp.where(diagonal, two, 0.0), axis=0, keepdims=True)
    used = (len(pairs) + count // 2) * BLOCK
    if part.shape[0] > used:
        pad = part.shape[0] - used
        part[pl.ds(used, pad), :] = jnp.zeros((pad, BLOCK), jnp.float32)

    pl.semaphore_wait(barrier, (n_in - 1) + (n_out - 1) + (ndp - 1))

    def remote(src, dst, send, recv, device):
        copy = pltpu.make_async_remote_copy(
            src_ref=src, dst_ref=dst, send_sem=send, recv_sem=recv,
            device_id=device, device_id_type=MESH,
        )
        copy.start()
        return copy

    class Path:
        def __init__(self, flip, start, length, bufs, sems):
            self.flip, self.start, self.length = flip, start, length
            self.got, self.hold, self.got2 = bufs
            self.s1, self.r1, self.s2, self.r2, self.s3, self.r3, self.s4, self.r4 = sems
            self.na, self.nb = (n_out, n_in) if flip else (n_in, n_out)
            self.ia, self.ib = (to, ti) if flip else (ti, to)
            self.to_a, self.to_b = (outer, inner) if flip else (inner, outer)
            self.turns = list(range(1, self.nb))[::-1] + [0]
            self.sent = []
            self.first, self.second, self.third, self.fourth = {}, {}, {}, {}

        def at(self, d, e):
            a, b = lax.rem(self.ia + d + self.na, self.na), lax.rem(self.ib + e + self.nb, self.nb)
            i, o = (b, a) if self.flip else (a, b)
            return pl.ds(
                pl.multiple_of((i * n_out + o) * chunk + self.start, 8), self.length
            )

        def begin(self, e):
            for d in range(1, self.na):
                self.first[d, e] = remote(
                    part.at[self.at(d, e), :], self.got.at[d - 1, e],
                    self.s1.at[d - 1, e], self.r1.at[d - 1, e], self.to_a(d),
                )

        def reduce(self, e):
            value = part[self.at(0, e), :]
            for d in range(1, self.na):
                self.first[d, e].wait_recv()
                value = value + self.got[d - 1, e]
            if e:
                self.hold[e - 1] = value
                self.second[e] = remote(
                    self.hold.at[e - 1], self.got2.at[e - 1], self.s2.at[e - 1],
                    self.r2.at[e - 1], self.to_b(e),
                )
            else:
                for e in range(1, self.nb):
                    self.second[e].wait_recv()
                    value = value + self.got2[e - 1]
                full[self.at(0, 0), :] = value
                mine = full.at[self.at(0, 0), :]
                for e in self.turns[:-1]:
                    self.third[e] = remote(
                        mine, mine, self.s3.at[e - 1], self.r3.at[e - 1], self.to_b(e)
                    )
                self.pass_on(0)

        def pass_on(self, e):
            if e:
                self.third[e].wait_recv()
            held = full.at[self.at(0, -e), :]
            for d in range(1, self.na):
                self.fourth[d, e] = remote(
                    held, held, self.s4.at[d - 1, e], self.r4.at[d - 1, e], self.to_a(d)
                )

        def finish(self):
            for copy in self.fourth.values():
                copy.wait_recv()

        def drain(self):
            for copies in (self.first, self.second, self.third, self.fourth):
                for copy in copies.values():
                    copy.wait_send()

    paths = [Path(False, 0, chunk - cut, (in_a, hold_a, out_a), sems_a)]
    if cut:
        paths.append(Path(True, chunk - cut, cut, (in_b, hold_b, out_b), sems_b))

    def together(name, lists):
        for k in range(max(len(turns) for turns in lists)):
            for path, turns in zip(paths, lists):
                if k < len(turns):
                    getattr(path, name)(turns[k])

    small = []
    for d in range(1, n_in):
        small.append(remote(dtile.at[0], dgot_in.at[d - 1], d1.at[d - 1], d2.at[d - 1], inner(d)))
    together("begin", [path.turns for path in paths])
    value = dtile[0]
    for d in range(1, n_in):
        small[d - 1].wait_recv()
        value = value + dgot_in[d - 1]
    dtile[1] = value
    wide = []
    for e in range(1, n_out):
        wide.append(remote(dtile.at[1], dgot_out.at[e - 1], d3.at[e - 1], d4.at[e - 1], outer(e)))
    together("reduce", [path.turns for path in paths])
    for e in range(1, n_out):
        wide[e - 1].wait_recv()
        value = value + dgot_out[e - 1]
    together("pass_on", [range(1, path.nb) for path in paths])
    for path in paths:
        path.finish()

    squared = jnp.zeros((BLOCK, BLOCK), jnp.float32)
    for m in range(count // 2):
        mixed = full[block(len(pairs) + m, 0)]
        squared = squared + jnp.where(diagonal, mixed + value[m : m + 1, :], 0.0)
    squared_norm = jnp.sum(jnp.sum(squared, axis=1, keepdims=True), axis=0, keepdims=True)
    divisor = jnp.sqrt(squared_norm) + norm_floor
    scale = 1.0 / (divisor * divisor)

    def place(i, j, block_value):
        gram[block(i, j)] = block_value
        put(gs, *block(i, j), block_value)

    for b, (i, j) in enumerate(pairs):
        scaled = full[block(b, 0)] * scale
        place(i, j, scaled)
        put(gs, *block(j, i), scaled.T)
        if i // (mtile // BLOCK) == j // (mtile // BLOCK):
            gram[block(j, i)] = scaled.T
    for m in range(count // 2):
        mixed = full[block(len(pairs) + m, 0)] * scale
        turned = mixed.T
        place(2 * m, 2 * m, jnp.where(above, mixed, turned))
        corner = jnp.where(diagonal, value[m : m + 1, :] * scale, turned)
        place(2 * m + 1, 2 * m + 1, jnp.where(here > there, mixed, corner))

    def product(a, b, at, columns):
        return (
            dot(a[0, at, :], b[1, :, columns]) + dot(a[1, at, :], b[0, :, columns])
        ) + dot(a[0, at, :], b[0, :, columns])

    def symmetric(a, b, target, ending):
        for r in range(0, order, mtile):
            at, columns = pl.ds(r, mtile), pl.ds(r, order - r)
            value = ending(r, at, columns, product(a, b, at, columns))
            put(target, at, columns, value)
            for c in range(r + mtile, order, mtile):
                put(target, pl.ds(c, mtile), at, value[:, c - r : c - r + mtile].T)

    def polynomial(r, at, columns, value):
        row = lax.broadcasted_iota(jnp.int32, value.shape, 0)
        column = lax.broadcasted_iota(jnp.int32, value.shape, 1)
        value = cubic_term * gram[at, columns] + quintic_term * value
        return value + jnp.where(row == column, linear_term, 0.0)

    def keep(r, at, columns, value):
        gram[at, columns] = value
        return value

    def plain(r, at, columns, value):
        return value

    running = p0s
    for turn in range(ITERS):
        target = running if turn == 0 else ps
        symmetric(gs, gs, target, polynomial)
        if turn + 1 < ITERS:
            symmetric(target, gs, qs, plain)
            symmetric(qs, target, gs, keep)
        if turn > 0:
            symmetric(running, target, spare, plain)
            running, spare = spare, running

    factor = update_gain * math.sqrt(max(rows * n_in * n_out, order)) / divisor
    last = []
    for c in range(0, order, mtile):
        for r in range(0, rows, tile):
            at, columns = pl.ds(r, tile), pl.ds(c, mtile)
            out_ref[dp, at, columns] = (
                product(gsplit, running, at, columns) * factor
            ).astype(jnp.bfloat16)
            done = out_ref.at[dp, at, columns]
            k = len(last) // max(ndp - 1, 1)
            for d in range(1, ndp):
                last.append(remote(done, done, s5.at[d - 1, k], r5.at[d - 1, k], sibling(d)))
    for path in paths:
        path.drain()
    for copy in small + wide:
        copy.wait_send()
    for copy in last:
        copy.wait()


def on_device(ndp, n, gradient):
    rows, order = gradient.shape[1], gradient.shape[2]
    n_in = 4 if n % 4 == 0 else 1
    n_out = n // n_in
    tile, mtile = min(256, rows), min(256, order)
    pieces = (rows // tile) * (order // mtile)
    count = order // BLOCK
    packed = count * count // 2 * BLOCK
    chunk = -(-packed // (8 * n)) * 8
    cut = chunk // CUT // 8 * 8 if n_in > 1 and n_out > 1 else 0
    total = chunk * n
    shape = (ndp, n_in, n_out, rows, order, chunk, cut)
    bf, f32 = jnp.bfloat16, jnp.float32
    inner, outer = max(n_in - 1, 1), max(n_out - 1, 1)
    dma = pltpu.SemaphoreType.DMA
    pair = pltpu.VMEM((2, order, order), bf)

    def buffers(na, nb, length):
        return [
            pltpu.VMEM((na, nb + 1, length, BLOCK), f32),
            pltpu.VMEM((nb, length, BLOCK), f32),
            pltpu.VMEM((nb, length, BLOCK), f32),
        ]

    def semaphores(na, nb):
        both = dma((na, nb + 1))
        return (both, both) + (dma((nb,)),) * 4 + (both, both)

    return pl.pallas_call(
        functools.partial(kernel, shape),
        out_shape=pltpu.VMEM((ndp, rows, order), bf),
        in_specs=[pl.BlockSpec(memory_space=pltpu.HBM)],
        out_specs=pl.BlockSpec(memory_space=pltpu.VMEM),
        scratch_shapes=[
            pltpu.VMEM((rows, order), f32),
            pltpu.VMEM((2, order, rows), bf),
            pltpu.VMEM((order, order), f32),
            pltpu.VMEM((total, BLOCK), f32),
            pltpu.VMEM((total, BLOCK), f32),
            pltpu.VMEM((order, order), f32),
            pair,
            pltpu.VMEM((2, rows, order), bf),
            pair, pair, pair, pair,
            pltpu.VMEM((2, 8, BLOCK), f32),
            pltpu.VMEM((inner, 8, BLOCK), f32),
            pltpu.VMEM((outer, 8, BLOCK), f32),
            *buffers(inner, outer, chunk - cut),
            *buffers(outer, inner, max(cut, 8)),
            dma((rows // tile,)),
            dma((inner,)), dma((inner,)), dma((outer,)), dma((outer,)),
            semaphores(inner, outer),
            semaphores(outer, inner),
            dma((max(ndp - 1, 1), pieces)),
            dma((max(ndp - 1, 1), pieces)),
        ],
        compiler_params=pltpu.CompilerParams(
            collective_id=0, has_side_effects=True, vmem_limit_bytes=62464 * 1024
        ),
    )(gradient[0])


def solution(mesh):
    body = functools.partial(on_device, mesh.shape["dp"], mesh.shape["tensor"])
    return jax.shard_map(
        body, mesh=mesh, in_specs=(P("dp", "tensor", None),),
        out_specs=P(None, "tensor", None), check_vma=False,
    )
```
